32 devices in a mesh: row: 16 (over z, x, core), chan: 2 (over y).
Axes of the slice: x: 2, y: 2, z: 4, core: 2. Of those that a mesh axis runs over, the one named last changes fastest.
Arguments:
- pair_rep: float32 [256, 256, 128], P('row', 'chan'), may hold values from -630 to 630
- residue_mask: int32 [256], replicated, may hold values from 0 to 1, as said below
- norm_gain: float32 [128], replicated, may hold values from 0.5 to 1.5
- norm_shift: float32 [128], replicated, may hold values from -3 to 3
- proj_weight: float32 [128, 512], replicated, may hold values from -4 to 4
- gate_shift: float32 [128], replicated, may hold values from -4 to 4
- bias_weight: float32 [128, 4], replicated, may hold values from -0.5 to 0.5
- out_weight: float32 [128, 128], replicated, may hold values from -0.5 to 0.5
Outputs:
- update: float32 [256, 256, 128], P('row', 'chan')
The draws below stay inside these ranges and needn't reach their ends.
Inputs may be any that keep to these rules, and one draw needn't show every extreme that they name: `residue_mask`: residue 0 is always valid.
All inputs are finite; a program needn't handle non-finite values.
Results may differ from the reference program's by a relative error of at most 0.012.
Values may be sent and summed in bfloat16 or wider, within the bound.
A program may use at most 64 MiB of HBM per device.

```python
import math
import jax
import jax.numpy as jnp
from jax import lax

C = 128
HEADS = 4
N = 256


def draw_pair_rep(key, part):
    key_noise, key_chan, key_pos = jax.random.split(key, 3)
    noise_draw = jnp.clip(jax.random.normal(key_noise, (N, N, C), jnp.float32), -6.0, 6.0)
    chan_scale = 10.0 ** jax.random.uniform(key_chan, (C,), jnp.float32)
    pos_scale = 10.0 ** jax.random.uniform(key_pos, (N, N, 1), jnp.float32)
    return noise_draw * chan_scale * pos_scale


def draw_proj_weight(key, part):
    key_base = jax.random.fold_in(key, 0)
    base = jnp.clip(jax.random.normal(key_base, (C, 4, HEADS, C // HEADS), jnp.float32), -4.0, 4.0) / math.sqrt(C)
    return base.reshape(C, 4 * C)


def draw_residue_mask(key, part):
    levels = jax.random.randint(key, (N,), 0, 4)
    return jnp.where(levels > 0, 1, 0).astype(jnp.int32).at[0].set(1)


def centred(own_key, extent, width, limit, dtype=jnp.bfloat16):
    result = width * jax.random.normal(own_key, extent, jnp.float32)
    return jnp.clip(result, min=-limit, max=limit).astype(dtype)


def setup_inputs(seed: int = 0) -> dict:
    splits = jax.random.split(jax.random.key(seed), 9)
    pair_rep = draw_pair_rep(jax.random.fold_in(splits[8], 71), 0)
    residue_mask = draw_residue_mask(jax.random.fold_in(splits[8], 71), 0)
    norm_gain = jnp.clip(1.0 + 0.1 * jax.random.normal(splits[2], (C,), jnp.float32), 0.5, 1.5)
    norm_shift = centred(splits[3], (C,), 0.5, 3.0, jnp.float32)
    proj_weight = draw_proj_weight(jax.random.fold_in(splits[8], 71), 0)
    gate_shift = centred(splits[5], (C,), 1.0, 4.0, jnp.float32)
    bias_weight = centred(splits[6], (C, HEADS), C ** -0.5, 0.5, jnp.float32)
    out_weight = centred(splits[7], (C, C), C ** -0.5, 0.5, jnp.float32)
    return {"pair_rep": pair_rep, "residue_mask": residue_mask, "norm_gain": norm_gain, "norm_shift": norm_shift, "proj_weight": proj_weight, "gate_shift": gate_shift, "bias_weight": bias_weight, "out_weight": out_weight}


def normalize(values, norm_gain, norm_shift):
    average = lax.optimization_barrier(jnp.mean(values, axis=-1, keepdims=True))
    centered = values - average
    variance = lax.optimization_barrier(jnp.mean(centered * centered, axis=-1, keepdims=True))
    return centered * lax.rsqrt(variance + 1e-05) * norm_gain + norm_shift

def reference(pair_rep, residue_mask, norm_gain, norm_shift, proj_weight, gate_shift, bias_weight, out_weight):
    highest = lax.Precision.HIGHEST
    head_dim = C // HEADS
    scaling = 1.0 / math.sqrt(head_dim)
    normed = normalize(pair_rep, norm_gain, norm_shift)
    pair_bias = jnp.einsum('jkc,ch->hjk', normed, bias_weight, precision=highest)
    valid_keys = (residue_mask > 0)[None, None, :]

    def one_row(pair_row):
        projected = jnp.dot(pair_row, proj_weight, precision=highest)
        query_half = (projected[:, :C] * scaling).astype(jnp.bfloat16)
        key_half = projected[:, C:2 * C].astype(jnp.bfloat16)
        value_half = projected[:, 2 * C:3 * C].astype(jnp.bfloat16)
        gates = projected[:, 3 * C:]
        queries = query_half.astype(jnp.float32).reshape(N, HEADS, head_dim)
        key_rows = key_half.astype(jnp.float32).reshape(N, HEADS, head_dim)
        value_rows = value_half.astype(jnp.float32).reshape(N, HEADS, head_dim)
        scores = jnp.einsum('jhd,khd->hjk', queries, key_rows, precision=highest) + pair_bias
        scores = jnp.where(valid_keys, scores, -1000000000.0)
        weights = jax.nn.softmax(scores, axis=-1)
        attended = jnp.einsum('hjk,khd->jhd', weights, value_rows, precision=highest).reshape(N, C)
        gated_rows = jax.nn.sigmoid(gates + gate_shift) * attended
        return jnp.dot(gated_rows, out_weight, precision=highest)
    return lax.map(one_row, normed)
```

```python
import functools
import math

import jax
import jax.numpy as jnp
from jax import lax
from jax.experimental import pallas as pl
from jax.experimental.pallas import tpu as pltpu
from jax.sharding import PartitionSpec as P

HEADS = 4
MESH = pl.DeviceIdType.MESH
NT = (((1,), (1,)), ((), ()))
NEVER = -1e30


def kernel(
    chans,
    group,
    x_ref,
    mask_ref,
    gain_ref,
    shift_ref,
    proj_ref,
    gate_ref,
    bw_ref,
    ow_ref,
    out_ref,
    xall,
    blocks,
    stage,
    own_bias,
    bias,
    w_own,
    w_kv,
    w_out,
    bw_pad,
    queries,
    gates,
    keys,
    values,
    result,
    x_send,
    x_recv,
    far_send,
    far_recv,
    near_send,
    near_recv,
    out_sem,
):
    rows, span, width = x_ref.shape
    total = chans * span
    head_dim = width // HEADS
    r = lax.axis_index("row")
    c = lax.axis_index("chan")
    hi = r // group
    lo = r % group
    is_home = (hi == c).astype(jnp.int32)

    barrier = pltpu.get_barrier_semaphore()
    for d in range(1, chans):
        pl.semaphore_signal(barrier, inc=1, device_id=(r, (c + d) % chans), device_id_type=MESH)
    for s in range(chans):

        @pl.when(jnp.logical_or(hi != c, c != s))
        def _():
            pl.semaphore_signal(barrier, inc=1, device_id=(c * group + lo, s), device_id_type=MESH)

    for d in range(1, group):
        pl.semaphore_signal(
            barrier, inc=1, device_id=(hi * group + (lo + d) % group, c), device_id_type=MESH
        )

    exp_scale = math.log2(math.e)
    proj = proj_ref[...]
    w_own[...] = proj.astype(jnp.bfloat16)
    w_kv[...] = proj[:, width : 3 * width].astype(jnp.bfloat16)
    w_out[...] = ow_ref[...].astype(jnp.bfloat16)
    bw_pad[...] = jnp.zeros_like(bw_pad)
    bw_pad[:, :HEADS] = bw_ref[...]
    bw_t = jnp.transpose(bw_pad[...])[:8].astype(jnp.bfloat16)
    gain = gain_ref[...].reshape(1, 1, width)
    shift = shift_ref[...].reshape(1, 1, width)

    step = 4 if rows % 4 == 0 else 1

    def norm_rows(n, carry):
        x = x_ref[pl.ds(n * step, step)]
        centered = x - jnp.mean(x, axis=-1, keepdims=True)
        variance = jnp.mean(centered * centered, axis=-1, keepdims=True)
        normed = (centered * lax.rsqrt(variance + 1e-05) * gain + shift).astype(jnp.bfloat16)
        for m in range(step):
            xall[n * step + m, c] = normed[m]
            local = lax.dot_general(bw_t, normed[m], NT, preferred_element_type=jnp.float32)
            stage[:, n * step + m, :] = local[:HEADS]
        return carry

    lax.fori_loop(0, rows // step, norm_rows, 0)
    own_bias[...] = stage[...].astype(jnp.bfloat16)

    @pl.when(hi == c)
    def _():
        blocks[lo, c] = stage[...].astype(jnp.bfloat16)

    pl.semaphore_wait(barrier, 2 * chans - 1 - is_home + group - 1)

    def far_copy(g, source):
        return pltpu.make_async_remote_copy(
            src_ref=own_bias,
            dst_ref=blocks.at[lo, source],
            send_sem=far_send.at[g],
            recv_sem=far_recv.at[source],
            device_id=(g * group + lo, hi),
            device_id_type=MESH,
        )

    for g in range(chans):

        @pl.when(jnp.logical_or(hi != c, hi != g))
        def _():
            far_copy(g, c).start()

    def x_copy(i, d, source):
        return pltpu.make_async_remote_copy(
            src_ref=xall.at[i, source],
            dst_ref=xall.at[i, source],
            send_sem=x_send.at[d - 1, i],
            recv_sem=x_recv.at[d - 1, i],
            device_id=(r, (c + d) % chans),
            device_id_type=MESH,
        )

    def send_row(i, carry):
        for d in range(1, chans):
            x_copy(i, d, c).start()
        return carry

    lax.fori_loop(0, rows, send_row, 0)

    scaling = exp_scale / math.sqrt(head_dim)

    def project_own(i, carry):
        full = jnp.dot(xall[i, c], w_own[...], preferred_element_type=jnp.float32)
        queries[i] = (full[:, :width] * scaling).astype(jnp.bfloat16)
        keys[i, c] = full[:, width : 2 * width].astype(jnp.bfloat16)
        values[i, c, :, :width] = full[:, 2 * width : 3 * width].astype(jnp.bfloat16)
        gates[i] = jax.nn.sigmoid(full[:, 3 * width :] + gate_ref[...])
        for s in range(chans):
            values[i, s, :, width:] = jnp.ones((span, width), jnp.bfloat16)
        return carry

    lax.fori_loop(0, rows, project_own, 0)

    for s in range(chans):

        @pl.when(jnp.logical_or(hi != c, c != s))
        def _():
            far_copy(s, s).wait_recv()

    def near_copy(d, source):
        return pltpu.make_async_remote_copy(
            src_ref=blocks.at[source],
            dst_ref=blocks.at[source],
            send_sem=near_send.at[d - 1],
            recv_sem=near_recv.at[d - 1],
            device_id=(hi * group + (lo + d) % group, c),
            device_id_type=MESH,
        )

    for d in range(1, group):
        near_copy(d, lo).start()
    for d in range(1, group):
        near_copy(d, (lo + group - d) % group).wait_recv()

    valid = mask_ref[...] > 0
    for s in range(chans):
        keep = valid[:, s * span : (s + 1) * span].reshape(1, 1, span)
        for h in range(HEADS):
            part = blocks[:, s, h].astype(jnp.float32) * exp_scale
            bias[h, :, :, s * span : (s + 1) * span] = jnp.where(keep, part, NEVER)

    lane = lax.broadcasted_iota(jnp.int32, (span, width), 1) // head_dim

    def out_copy(i):
        return pltpu.make_async_copy(result.at[i], out_ref.at[i], out_sem.at[i])

    def attend(i, carry):
        for d in range(1, chans):
            source = (c + chans - d) % chans
            x_copy(i, d, source).wait_recv()
            kv = jnp.dot(xall[i, source], w_kv[...], preferred_element_type=jnp.float32)
            keys[i, source] = kv[:, :width].astype(jnp.bfloat16)
            values[i, source, :, :width] = kv[:, width:].astype(jnp.bfloat16)
        query = queries[i]
        key = keys[i].reshape(total, width)
        value = values[i].reshape(total, 2 * width)
        top = jnp.zeros((span, width), jnp.float32)
        norm = jnp.zeros((span, width), jnp.float32)
        for h in range(HEADS):
            mine = jnp.where(lane == h, query, jnp.zeros_like(query))
            scores = lax.dot_general(mine, key, NT, preferred_element_type=jnp.float32)
            scores = scores + bias[h].reshape(span, total)
            peak = jnp.max(scores, axis=-1, keepdims=True)
            weights = jnp.exp2(scores - peak).astype(jnp.bfloat16)
            both = jnp.dot(weights, value, preferred_element_type=jnp.float32)
            top = jnp.where(lane == h, both[:, :width], top)
            norm = jnp.where(lane == h, both[:, width:], norm)
        gated = gates[i] * (top / norm)
        result[i] = jnp.dot(
            gated.astype(jnp.bfloat16), w_out[...], preferred_element_type=jnp.float32
        )
        out_copy(i).start()
        return carry

    lax.fori_loop(0, rows, attend, 0)

    for g in range(chans):

        @pl.when(jnp.logical_or(hi != c, hi != g))
        def _():
            far_copy(g, c).wait_send()

    for d in range(1, group):
        near_copy(d, lo).wait_send()

    def finish(i, carry):
        for d in range(1, chans):
            x_copy(i, d, c).wait_send()
        out_copy(i).wait()
        return carry

    lax.fori_loop(0, rows, finish, 0)


def body(
    chans,
    pair_rep,
    residue_mask,
    norm_gain,
    norm_shift,
    proj_weight,
    gate_shift,
    bias_weight,
    out_weight,
):
    rows, span, width = pair_rep.shape
    group = span // rows
    total = chans * span
    vmem = pl.BlockSpec(memory_space=pltpu.VMEM)
    half = jnp.bfloat16
    full = jnp.float32
    return pl.pallas_call(
        functools.partial(kernel, chans, group),
        out_shape=jax.ShapeDtypeStruct((rows, span, width), full),
        in_specs=[vmem] * 8,
        out_specs=pl.BlockSpec(memory_space=pl.ANY),
        scratch_shapes=[
            pltpu.VMEM((rows, chans, span, width), half),
            pltpu.VMEM((group, chans, HEADS, rows, span), half),
            pltpu.VMEM((HEADS, rows, span), full),
            pltpu.VMEM((HEADS, rows, span), half),
            pltpu.VMEM((HEADS, group, rows, total), full),
            pltpu.VMEM((width, 4 * width), half),
            pltpu.VMEM((width, 2 * width), half),
            pltpu.VMEM((width, width), half),
            pltpu.VMEM((width, width), full),
            pltpu.VMEM((rows, span, width), half),
            pltpu.VMEM((rows, span, width), full),
            pltpu.VMEM((rows, chans, span, width), half),
            pltpu.VMEM((rows, chans, span, 2 * width), half),
            pltpu.VMEM((rows, span, width), full),
            pltpu.SemaphoreType.DMA((chans - 1, rows)),
            pltpu.SemaphoreType.DMA((chans - 1, rows)),
            pltpu.SemaphoreType.DMA((chans,)),
            pltpu.SemaphoreType.DMA((chans,)),
            pltpu.SemaphoreType.DMA((group - 1,)),
            pltpu.SemaphoreType.DMA((group - 1,)),
            pltpu.SemaphoreType.DMA((rows,)),
        ],
        compiler_params=pltpu.CompilerParams(
            collective_id=0, has_side_effects=True, vmem_limit_bytes=56 * 1024 * 1024
        ),
    )(
        pair_rep,
        residue_mask.reshape(1, total),
        norm_gain.reshape(1, width),
        norm_shift.reshape(1, width),
        proj_weight,
        gate_shift.reshape(1, width),
        bias_weight,
        out_weight,
    )


def solution(mesh):
    return jax.shard_map(
        functools.partial(body, mesh.shape["chan"]),
        mesh=mesh,
        in_specs=(P("row", "chan", None), P(), P(), P(), P(), P(), P(), P()),
        out_specs=P("row", "chan", None),
        check_vma=False,
    )
```

```python
import functools
import math

import jax
import jax.numpy as jnp
from jax import lax
from jax.experimental import pallas as pl
from jax.experimental.pallas import tpu as pltpu
from jax.sharding import PartitionSpec as P

HEADS = 4
MESH = pl.DeviceIdType.MESH
NT = (((1,), (1,)), ((), ()))
NEVER = -1e30


def halves(value):
    high = value.astype(jnp.bfloat16)
    return high, (value - high.astype(jnp.float32)).astype(jnp.bfloat16)


def kernel(
    chans,
    group,
    x_ref,
    mask_ref,
    gain_ref,
    shift_ref,
    proj_ref,
    gate_ref,
    bw_ref,
    ow_ref,
    out_ref,
    xall,
    blocks,
    stage,
    own_bias,
    bias,
    w_own,
    w_kv,
    w_out,
    xlow,
    queries,
    gates,
    keys,
    values,
    result,
    x_send,
    x_recv,
    far_send,
    far_recv,
    near_send,
    near_recv,
    out_sem,
):
    rows, span, width = x_ref.shape
    total = chans * span
    head_dim = width // HEADS
    r = lax.axis_index("row")
    c = lax.axis_index("chan")
    hi = r // group
    lo = r % group
    is_home = (hi == c).astype(jnp.int32)

    barrier = pltpu.get_barrier_semaphore()
    for d in range(1, chans):
        pl.semaphore_signal(barrier, inc=1, device_id=(r, (c + d) % chans), device_id_type=MESH)
    for s in range(chans):

        @pl.when(jnp.logical_or(hi != c, c != s))
        def _():
            pl.semaphore_signal(barrier, inc=1, device_id=(c * group + lo, s), device_id_type=MESH)

    for d in range(1, group):
        pl.semaphore_signal(
            barrier, inc=1, device_id=(hi * group + (lo + d) % group, c), device_id_type=MESH
        )

    exp_scale = math.log2(math.e)
    proj_high, proj_low = halves(proj_ref[...])
    w_own[:width] = proj_high
    w_own[width : 2 * width] = proj_high
    w_own[2 * width :] = proj_low
    w_kv[:width] = proj_high[:, width : 3 * width]
    w_kv[width:] = proj_low[:, width : 3 * width]
    out_high, out_low = halves(ow_ref[...])
    w_out[:width] = out_high
    w_out[width : 2 * width] = out_high
    w_out[2 * width :] = out_low
    bw_high, bw_low = halves(bw_ref[...])
    bw_t = jnp.concatenate([bw_high, bw_high, bw_low], axis=1)
    gain = gain_ref[...].reshape(1, 1, width)
    shift = shift_ref[...].reshape(1, 1, width)

    step = 4 if rows % 4 == 0 else 1

    def norm_rows(n, carry):
        x = x_ref[pl.ds(n * step, step)]
        centered = x - jnp.mean(x, axis=-1, keepdims=True)
        variance = jnp.mean(centered * centered, axis=-1, keepdims=True)
        high, low = halves(centered * lax.rsqrt(variance + 1e-05) * gain + shift)
        for m in range(step):
            xall[n * step + m, c] = high[m]
            xlow[n * step + m] = low[m]
            local = lax.dot_general(
                bw_t,
                jnp.concatenate([high[m], low[m], high[m]], axis=1),
                NT,
                preferred_element_type=jnp.float32,
            )
            stage[:, n * step + m, :] = local[:HEADS] * exp_scale
        return carry

    lax.fori_loop(0, rows // step, norm_rows, 0)
    own_bias[...] = stage[...].astype(jnp.bfloat16)

    @pl.when(hi == c)
    def _():
        blocks[lo, c] = stage[...].astype(jnp.bfloat16)

    pl.semaphore_wait(barrier, 2 * chans - 1 - is_home + group - 1)

    def far_copy(g, source):
        return pltpu.make_async_remote_copy(
            src_ref=own_bias,
            dst_ref=blocks.at[lo, source],
            send_sem=far_send.at[g],
            recv_sem=far_recv.at[source],
            device_id=(g * group + lo, hi),
            device_id_type=MESH,
        )

    for g in range(chans):

        @pl.when(jnp.logical_or(hi != c, hi != g))
        def _():
            far_copy(g, c).start()

    def x_copy(i, d, source):
        return pltpu.make_async_remote_copy(
            src_ref=xall.at[i, source],
            dst_ref=xall.at[i, source],
            send_sem=x_send.at[d - 1, i],
            recv_sem=x_recv.at[d - 1, i],
            device_id=(r, (c + d) % chans),
            device_id_type=MESH,
        )

    def send_row(i, carry):
        for d in range(1, chans):
            x_copy(i, d, c).start()
        return carry

    lax.fori_loop(0, rows, send_row, 0)

    scaling = exp_scale / math.sqrt(head_dim)

    def project_own(i, carry):
        high = xall[i, c]
        full = jnp.dot(
            jnp.concatenate([high, xlow[i], high], axis=1),
            w_own[...],
            preferred_element_type=jnp.float32,
        )
        queries[i] = (full[:, :width] * scaling).astype(jnp.bfloat16)
        keys[i, c] = full[:, width : 2 * width].astype(jnp.bfloat16)
        values[i, c, :, :width] = full[:, 2 * width : 3 * width].astype(jnp.bfloat16)
        gates[i] = jax.nn.sigmoid(full[:, 3 * width :] + gate_ref[...])
        for s in range(chans):
            values[i, s, :, width:] = jnp.ones((span, width), jnp.bfloat16)
        return carry

    lax.fori_loop(0, rows, project_own, 0)

    for s in range(chans):

        @pl.when(jnp.logical_or(hi != c, c != s))
        def _():
            far_copy(s, s).wait_recv()

    def near_copy(d, source):
        return pltpu.make_async_remote_copy(
            src_ref=blocks.at[source],
            dst_ref=blocks.at[source],
            send_sem=near_send.at[d - 1],
            recv_sem=near_recv.at[d - 1],
            device_id=(hi * group + (lo + d) % group, c),
            device_id_type=MESH,
        )

    for d in range(1, group):
        near_copy(d, lo).start()

    def project_other(i, carry):
        for d in range(1, chans):
            source = (c + chans - d) % chans
            x_copy(i, d, source).wait_recv()
            other = xall[i, source]
            kv = jnp.dot(
                jnp.concatenate([other, other], axis=1),
                w_kv[...],
                preferred_element_type=jnp.float32,
            )
            keys[i, source] = kv[:, :width].astype(jnp.bfloat16)
            values[i, source, :, :width] = kv[:, width:].astype(jnp.bfloat16)
        return carry

    early = rows // 2
    lax.fori_loop(0, early, project_other, 0)

    for d in range(1, group):
        near_copy(d, (lo + group - d) % group).wait_recv()

    valid = mask_ref[...] > 0
    for s in range(chans):
        keep = valid[:, s * span : (s + 1) * span].reshape(1, 1, span)
        for h in range(HEADS):
            part = blocks[:, s, h].astype(jnp.float32)
            bias[h, :, :, s * span : (s + 1) * span] = jnp.where(keep, part, NEVER)

    lane = lax.broadcasted_iota(jnp.int32, (span, width), 1) // head_dim

    def out_copy(i):
        return pltpu.make_async_copy(result.at[i], out_ref.at[i], out_sem.at[i])

    def attend(i, carry):
        query = queries[i]
        key = keys[i].reshape(total, width)
        value = values[i].reshape(total, 2 * width)
        top = jnp.zeros((span, width), jnp.float32)
        norm = jnp.zeros((span, width), jnp.float32)
        for h in range(HEADS):
            mine = jnp.where(lane == h, query, jnp.zeros_like(query))
            scores = lax.dot_general(mine, key, NT, preferred_element_type=jnp.float32)
            scores = scores + bias[h].reshape(span, total)
            peak = jnp.max(scores, axis=-1, keepdims=True)
            weights = jnp.exp2(scores - peak).astype(jnp.bfloat16)
            both = jnp.dot(weights, value, preferred_element_type=jnp.float32)
            top = jnp.where(lane == h, both[:, :width], top)
            norm = jnp.where(lane == h, both[:, width:], norm)
        high, low = halves(gates[i] * (top / norm))
        result[i] = jnp.dot(
            jnp.concatenate([high, low, high], axis=1),
            w_out[...],
            preferred_element_type=jnp.float32,
        )
        out_copy(i).start()
        return carry

    def attend_ahead(i, carry):
        project_other(i + early, carry)
        return attend(i, carry)

    lax.fori_loop(0, rows - early, attend_ahead, 0)
    lax.fori_loop(rows - early, rows, attend, 0)

    for g in range(chans):

        @pl.when(jnp.logical_or(hi != c, hi != g))
        def _():
            far_copy(g, c).wait_send()

    for d in range(1, group):
        near_copy(d, lo).wait_send()

    def finish(i, carry):
        for d in range(1, chans):
            x_copy(i, d, c).wait_send()
        out_copy(i).wait()
        return carry

    lax.fori_loop(0, rows, finish, 0)


def body(
    chans,
    pair_rep,
    residue_mask,
    norm_gain,
    norm_shift,
    proj_weight,
    gate_shift,
    bias_weight,
    out_weight,
):
    rows, span, width = pair_rep.shape
    group = span // rows
    total = chans * span
    vmem = pl.BlockSpec(memory_space=pltpu.VMEM)
    half = jnp.bfloat16
    full = jnp.float32
    return pl.pallas_call(
        functools.partial(kernel, chans, group),
        out_shape=jax.ShapeDtypeStruct((rows, span, width), full),
        in_specs=[vmem] * 8,
        out_specs=pl.BlockSpec(memory_space=pl.ANY),
        scratch_shapes=[
            pltpu.VMEM((rows, chans, span, width), half),
            pltpu.VMEM((group, chans, HEADS, rows, span), half),
            pltpu.VMEM((HEADS, rows, span), full),
            pltpu.VMEM((HEADS, rows, span), half),
            pltpu.VMEM((HEADS, group, rows, total), full),
            pltpu.VMEM((3 * width, 4 * width), half),
            pltpu.VMEM((2 * width, 2 * width), half),
            pltpu.VMEM((3 * width, width), half),
            pltpu.VMEM((rows, span, width), half),
            pltpu.VMEM((rows, span, width), half),
            pltpu.VMEM((rows, span, width), full),
            pltpu.VMEM((rows, chans, span, width), half),
            pltpu.VMEM((rows, chans, span, 2 * width), half),
            pltpu.VMEM((rows, span, width), full),
            pltpu.SemaphoreType.DMA((chans - 1, rows)),
            pltpu.SemaphoreType.DMA((chans - 1, rows)),
            pltpu.SemaphoreType.DMA((chans,)),
            pltpu.SemaphoreType.DMA((chans,)),
            pltpu.SemaphoreType.DMA((group - 1,)),
            pltpu.SemaphoreType.DMA((group - 1,)),
            pltpu.SemaphoreType.DMA((rows,)),
        ],
        compiler_params=pltpu.CompilerParams(
            collective_id=0, has_side_effects=True, vmem_limit_bytes=56 * 1024 * 1024
        ),
    )(
        pair_rep,
        residue_mask.reshape(1, total),
        norm_gain.reshape(1, width),
        norm_shift.reshape(1, width),
        proj_weight,
        gate_shift.reshape(1, width),
        bias_weight.T,
        out_weight,
    )


def solution(mesh):
    return jax.shard_map(
        functools.partial(body, mesh.shape["chan"]),
        mesh=mesh,
        in_specs=(P("row", "chan", None), P(), P(), P(), P(), P(), P(), P()),
        out_specs=P("row", "chan", None),
        check_vma=False,
    )
```

```python
import functools
import math

import jax
import jax.numpy as jnp
from jax import lax
from jax.experimental import pallas as pl
from jax.experimental.pallas import tpu as pltpu
from jax.sharding import PartitionSpec as P

HEADS = 4
MESH = pl.DeviceIdType.MESH
NT = (((1,), (1,)), ((), ()))
NEVER = -1e30


def halves(value):
    high = value.astype(jnp.bfloat16)
    return high, (value - high.astype(jnp.float32)).astype(jnp.bfloat16)


def kernel(
    chans,
    group,
    x_ref,
    mask_ref,
    gain_ref,
    shift_ref,
    proj_ref,
    gate_ref,
    bw_ref,
    ow_ref,
    out_ref,
    xall,
    blocks,
    stage,
    own_bias,
    bias,
    w_own,
    w_kv,
    w_out,
    xlow,
    queries,
    gates,
    keys,
    values,
    result,
    x_send,
    x_recv,
    far_send,
    far_recv,
    near_send,
    near_recv,
    out_sem,
):
    rows, span, width = x_ref.shape
    total = chans * span
    head_dim = width // HEADS
    r = lax.axis_index("row")
    c = lax.axis_index("chan")
    hi = r // group
    lo = r % group
    is_home = (hi == c).astype(jnp.int32)

    barrier = pltpu.get_barrier_semaphore()
    for d in range(1, chans):
        pl.semaphore_signal(barrier, inc=1, device_id=(r, (c + d) % chans), device_id_type=MESH)
    for s in range(chans):

        @pl.when(jnp.logical_or(hi != c, c != s))
        def _():
            pl.semaphore_signal(barrier, inc=1, device_id=(c * group + lo, s), device_id_type=MESH)

    for d in range(1, group):
        pl.semaphore_signal(
            barrier, inc=1, device_id=(hi * group + (lo + d) % group, c), device_id_type=MESH
        )

    exp_scale = math.log2(math.e)
    proj_high, proj_low = halves(proj_ref[...])
    w_own[:width] = proj_high
    w_own[width : 2 * width] = proj_high
    w_own[2 * width :] = proj_low
    w_kv[:width] = proj_high[:, width : 3 * width]
    w_kv[width:] = proj_low[:, width : 3 * width]
    out_high, out_low = halves(ow_ref[...])
    w_out[:width] = out_high
    w_out[width : 2 * width] = out_high
    w_out[2 * width :] = out_low
    bw_high, bw_low = halves(bw_ref[...])
    bw_t = jnp.concatenate([bw_high, bw_high, bw_low], axis=1)
    gain = gain_ref[...].reshape(1, 1, width)
    shift = shift_ref[...].reshape(1, 1, width)

    step = 4 if rows % 4 == 0 else 1

    def norm_rows(n, carry):
        x = x_ref[pl.ds(n * step, step)]
        centered = x - jnp.mean(x, axis=-1, keepdims=True)
        variance = jnp.mean(centered * centered, axis=-1, keepdims=True)
        high, low = halves(centered * lax.rsqrt(variance + 1e-05) * gain + shift)
        for m in range(step):
            xall[n * step + m, c] = high[m]
            xlow[n * step + m] = low[m]
            local = lax.dot_general(
                bw_t,
                jnp.concatenate([high[m], low[m], high[m]], axis=1),
                NT,
                preferred_element_type=jnp.float32,
            )
            stage[:, n * step + m, :] = local[:HEADS] * exp_scale
        return carry

    lax.fori_loop(0, rows // step, norm_rows, 0)
    own_bias[...] = stage[...].astype(jnp.bfloat16)

    @pl.when(hi == c)
    def _():
        blocks[lo, c] = stage[...].astype(jnp.bfloat16)

    pl.semaphore_wait(barrier, 2 * chans - 1 - is_home + group - 1)

    def far_copy(g, source):
        return pltpu.make_async_remote_copy(
            src_ref=own_bias,
            dst_ref=blocks.at[lo, source],
            send_sem=far_send.at[g],
            recv_sem=far_recv.at[source],
            device_id=(g * group + lo, hi),
            device_id_type=MESH,
        )

    for g in range(chans):

        @pl.when(jnp.logical_or(hi != c, hi != g))
        def _():
            far_copy(g, c).start()

    def x_copy(i, d, source):
        return pltpu.make_async_remote_copy(
            src_ref=xall.at[i, source],
            dst_ref=xall.at[i, source],
            send_sem=x_send.at[d - 1, i],
            recv_sem=x_recv.at[d - 1, i],
            device_id=(r, (c + d) % chans),
            device_id_type=MESH,
        )

    def send_row(i, carry):
        for d in range(1, chans):
            x_copy(i, d, c).start()
        return carry

    early = rows // 4
    lax.fori_loop(0, early, send_row, 0)

    scaling = exp_scale / math.sqrt(head_dim)

    def project_own(i, carry):
        high = xall[i, c]
        full = jnp.dot(
            jnp.concatenate([high, xlow[i], high], axis=1),
            w_own[...],
            preferred_element_type=jnp.float32,
        )
        queries[i] = (full[:, :width] * scaling).astype(jnp.bfloat16)
        keys[i, c] = full[:, width : 2 * width].astype(jnp.bfloat16)
        values[i, c, :, :width] = full[:, 2 * width : 3 * width].astype(jnp.bfloat16)
        gates[i] = jax.nn.sigmoid(full[:, 3 * width :] + gate_ref[...])
        for s in range(chans):
            values[i, s, :, width:] = jnp.ones((span, width), jnp.bfloat16)
        return carry

    lax.fori_loop(0, rows, project_own, 0)

    for s in range(chans):

        @pl.when(jnp.logical_or(hi != c, c != s))
        def _():
            far_copy(s, s).wait_recv()

    def near_copy(d, source):
        return pltpu.make_async_remote_copy(
            src_ref=blocks.at[source],
            dst_ref=blocks.at[source],
            send_sem=near_send.at[d - 1],
            recv_sem=near_recv.at[d - 1],
            device_id=(hi * group + (lo + d) % group, c),
            device_id_type=MESH,
        )

    for d in range(1, group):
        near_copy(d, lo).start()
    lax.fori_loop(early, rows, send_row, 0)

    def project_other(i, carry):
        for d in range(1, chans):
            source = (c + chans - d) % chans
            x_copy(i, d, source).wait_recv()
            other = xall[i, source]
            kv = jnp.dot(
                jnp.concatenate([other, other], axis=1),
                w_kv[...],
                preferred_element_type=jnp.float32,
            )
            keys[i, source] = kv[:, :width].astype(jnp.bfloat16)
            values[i, source, :, :width] = kv[:, width:].astype(jnp.bfloat16)
        return carry

    lax.fori_loop(0, early, project_other, 0)

    for d in range(1, group):
        near_copy(d, (lo + group - d) % group).wait_recv()

    valid = mask_ref[...] > 0
    for s in range(chans):
        keep = valid[:, s * span : (s + 1) * span].reshape(1, 1, span)
        for h in range(HEADS):
            part = blocks[:, s, h].astype(jnp.float32)
            bias[h, :, :, s * span : (s + 1) * span] = jnp.where(keep, part, NEVER)

    lane = lax.broadcasted_iota(jnp.int32, (span, width), 1) // head_dim

    def out_copy(i):
        return pltpu.make_async_copy(result.at[i], out_ref.at[i], out_sem.at[i])

    def attend(i, carry):
        query = queries[i]
        key = keys[i].reshape(total, width)
        value = values[i].reshape(total, 2 * width)
        top = jnp.zeros((span, width), jnp.float32)
        norm = jnp.zeros((span, width), jnp.float32)
        for h in range(HEADS):
            mine = jnp.where(lane == h, query, jnp.zeros_like(query))
            scores = lax.dot_general(mine, key, NT, preferred_element_type=jnp.float32)
            scores = scores + bias[h].reshape(span, total)
            peak = jnp.max(scores, axis=-1, keepdims=True)
            weights = jnp.exp2(scores - peak).astype(jnp.bfloat16)
            both = jnp.dot(weights, value, preferred_element_type=jnp.float32)
            top = jnp.where(lane == h, both[:, :width], top)
            norm = jnp.where(lane == h, both[:, width:], norm)
        high, low = halves(gates[i] * (top / norm))
        result[i] = jnp.dot(
            jnp.concatenate([high, low, high], axis=1),
            w_out[...],
            preferred_element_type=jnp.float32,
        )
        out_copy(i).start()
        return carry

    def attend_ahead(i, carry):
        project_other(i + early, carry)
        return attend(i, carry)

    lax.fori_loop(0, rows - early, attend_ahead, 0)
    lax.fori_loop(rows - early, rows, attend, 0)

    for g in range(chans):

        @pl.when(jnp.logical_or(hi != c, hi != g))
        def _():
            far_copy(g, c).wait_send()

    for d in range(1, group):
        near_copy(d, lo).wait_send()

    def finish(i, carry):
        for d in range(1, chans):
            x_copy(i, d, c).wait_send()
        out_copy(i).wait()
        return carry

    lax.fori_loop(0, rows, finish, 0)


def body(
    chans,
    pair_rep,
    residue_mask,
    norm_gain,
    norm_shift,
    proj_weight,
    gate_shift,
    bias_weight,
    out_weight,
):
    rows, span, width = pair_rep.shape
    group = span // rows
    total = chans * span
    vmem = pl.BlockSpec(memory_space=pltpu.VMEM)
    half = jnp.bfloat16
    full = jnp.float32
    return pl.pallas_call(
        functools.partial(kernel, chans, group),
        out_shape=jax.ShapeDtypeStruct((rows, span, width), full),
        in_specs=[vmem] * 8,
        out_specs=pl.BlockSpec(memory_space=pl.ANY),
        scratch_shapes=[
            pltpu.VMEM((rows, chans, span, width), half),
            pltpu.VMEM((group, chans, HEADS, rows, span), half),
            pltpu.VMEM((HEADS, rows, span), full),
            pltpu.VMEM((HEADS, rows, span), half),
            pltpu.VMEM((HEADS, group, rows, total), full),
            pltpu.VMEM((3 * width, 4 * width), half),
            pltpu.VMEM((2 * width, 2 * width), half),
            pltpu.VMEM((3 * width, width), half),
            pltpu.VMEM((rows, span, width), half),
            pltpu.VMEM((rows, span, width), half),
            pltpu.VMEM((rows, span, width), full),
            pltpu.VMEM((rows, chans, span, width), half),
            pltpu.VMEM((rows, chans, span, 2 * width), half),
            pltpu.VMEM((rows, span, width), full),
            pltpu.SemaphoreType.DMA((chans - 1, rows)),
            pltpu.SemaphoreType.DMA((chans - 1, rows)),
            pltpu.SemaphoreType.DMA((chans,)),
            pltpu.SemaphoreType.DMA((chans,)),
            pltpu.SemaphoreType.DMA((group - 1,)),
            pltpu.SemaphoreType.DMA((group - 1,)),
            pltpu.SemaphoreType.DMA((rows,)),
        ],
        compiler_params=pltpu.CompilerParams(
            collective_id=0, has_side_effects=True, vmem_limit_bytes=56 * 1024 * 1024
        ),
    )(
        pair_rep,
        residue_mask.reshape(1, total),
        norm_gain.reshape(1, width),
        norm_shift.reshape(1, width),
        proj_weight,
        gate_shift.reshape(1, width),
        bias_weight.T,
        out_weight,
    )


def solution(mesh):
    return jax.shard_map(
        functools.partial(body, mesh.shape["chan"]),
        mesh=mesh,
        in_specs=(P("row", "chan", None), P(), P(), P(), P(), P(), P(), P()),
        out_specs=P("row", "chan", None),
        check_vma=False,
    )
```

```python
import functools
import math

import jax
import jax.numpy as jnp
from jax import lax
from jax.experimental import pallas as pl
from jax.experimental.pallas import tpu as pltpu
from jax.sharding import PartitionSpec as P

HEADS = 4
MESH = pl.DeviceIdType.MESH
NT = (((1,), (1,)), ((), ()))
NEVER = -1e30


def halves(value):
    high = value.astype(jnp.bfloat16)
    return high, (value - high.astype(jnp.float32)).astype(jnp.bfloat16)


def kernel(
    chans,
    group,
    x_ref,
    mask_ref,
    gain_ref,
    shift_ref,
    proj_ref,
    gate_ref,
    bw_ref,
    ow_ref,
    out_ref,
    xall,
    blocks,
    stage,
    own_bias,
    bias,
    w_own,
    w_kv,
    w_out,
    xlow,
    queries,
    gates,
    keys,
    values,
    result,
    x_send,
    x_recv,
    far_send,
    far_recv,
    near_send,
    near_recv,
    out_sem,
):
    rows, span, width = x_ref.shape
    total = chans * span
    head_dim = width // HEADS
    r = lax.axis_index("row")
    c = lax.axis_index("chan")
    hi = r // group
    lo = r % group
    is_home = (hi == c).astype(jnp.int32)

    barrier = pltpu.get_barrier_semaphore()
    for d in range(1, chans):
        pl.semaphore_signal(barrier, inc=1, device_id=(r, (c + d) % chans), device_id_type=MESH)
    for s in range(chans):

        @pl.when(jnp.logical_or(hi != c, c != s))
        def _():
            pl.semaphore_signal(barrier, inc=1, device_id=(c * group + lo, s), device_id_type=MESH)

    for d in range(1, group):
        pl.semaphore_signal(
            barrier, inc=1, device_id=(hi * group + (lo + d) % group, c), device_id_type=MESH
        )

    exp_scale = math.log2(math.e)
    proj_high, proj_low = halves(proj_ref[...])
    w_own[:width] = proj_high
    w_own[width : 2 * width] = proj_high
    w_own[2 * width :] = proj_low
    w_kv[:width] = proj_high[:, width : 3 * width]
    w_kv[width:] = proj_low[:, width : 3 * width]
    out_high, out_low = halves(ow_ref[...])
    w_out[:width] = out_high
    w_out[width : 2 * width] = out_high
    w_out[2 * width :] = out_low
    bw_high, bw_low = halves(bw_ref[...])
    bw_t = jnp.concatenate([bw_high, bw_high, bw_low], axis=1)
    gain = gain_ref[...].reshape(1, 1, width)
    shift = shift_ref[...].reshape(1, 1, width)

    step = 4 if rows % 4 == 0 else 1

    def norm_rows(n, carry):
        x = x_ref[pl.ds(n * step, step)]
        centered = x - jnp.mean(x, axis=-1, keepdims=True)
        variance = jnp.mean(centered * centered, axis=-1, keepdims=True)
        high, low = halves(centered * lax.rsqrt(variance + 1e-05) * gain + shift)
        for m in range(step):
            xall[n * step + m, c] = high[m]
            xlow[n * step + m] = low[m]
            local = lax.dot_general(
                bw_t,
                jnp.concatenate([high[m], low[m], high[m]], axis=1),
                NT,
                preferred_element_type=jnp.float32,
            )
            stage[:, n * step + m, :] = local[:HEADS] * exp_scale
        return carry

    lax.fori_loop(0, rows // step, norm_rows, 0)
    own_bias[...] = stage[...].astype(jnp.bfloat16)

    @pl.when(hi == c)
    def _():
        blocks[lo, c] = stage[...].astype(jnp.bfloat16)

    pl.semaphore_wait(barrier, 2 * chans - 1 - is_home + group - 1)

    def far_copy(g, source):
        return pltpu.make_async_remote_copy(
            src_ref=own_bias,
            dst_ref=blocks.at[lo, source],
            send_sem=far_send.at[g],
            recv_sem=far_recv.at[source],
            device_id=(g * group + lo, hi),
            device_id_type=MESH,
        )

    for g in range(chans):

        @pl.when(jnp.logical_or(hi != c, hi != g))
        def _():
            far_copy(g, c).start()

    def x_copy(i, d, source):
        return pltpu.make_async_remote_copy(
            src_ref=xall.at[i, source],
            dst_ref=xall.at[i, source],
            send_sem=x_send.at[d - 1, i],
            recv_sem=x_recv.at[d - 1, i],
            device_id=(r, (c + d) % chans),
            device_id_type=MESH,
        )

    def send_row(i, carry):
        for d in range(1, chans):
            x_copy(i, d, c).start()
        return carry

    lax.fori_loop(0, rows, send_row, 0)

    scaling = exp_scale / math.sqrt(head_dim)

    def project_own(i, carry):
        high = xall[i, c]
        full = jnp.dot(
            jnp.concatenate([high, xlow[i], high], axis=1),
            w_own[...],
            preferred_element_type=jnp.float32,
        )
        queries[i] = (full[:, :width] * scaling).astype(jnp.bfloat16)
        keys[i, c] = full[:, width : 2 * width].astype(jnp.bfloat16)
        values[i, c, :, :width] = full[:, 2 * width : 3 * width].astype(jnp.bfloat16)
        gates[i] = jax.nn.sigmoid(full[:, 3 * width :] + gate_ref[...])
        for s in range(chans):
            values[i, s, :, width:] = jnp.ones((span, width), jnp.bfloat16)
        return carry

    lax.fori_loop(0, rows, project_own, 0)

    for s in range(chans):

        @pl.when(jnp.logical_or(hi != c, c != s))
        def _():
            far_copy(s, s).wait_recv()

    def near_copy(d, source):
        return pltpu.make_async_remote_copy(
            src_ref=blocks.at[source],
            dst_ref=blocks.at[source],
            send_sem=near_send.at[d - 1],
            recv_sem=near_recv.at[d - 1],
            device_id=(hi * group + (lo + d) % group, c),
            device_id_type=MESH,
        )

    for d in range(1, group):
        near_copy(d, lo).start()

    def project_other(i, carry):
        for d in range(1, chans):
            source = (c + chans - d) % chans
            x_copy(i, d, source).wait_recv()
            other = xall[i, source]
            kv = jnp.dot(
                jnp.concatenate([other, other], axis=1),
                w_kv[...],
                preferred_element_type=jnp.float32,
            )
            keys[i, source] = kv[:, :width].astype(jnp.bfloat16)
            values[i, source, :, :width] = kv[:, width:].astype(jnp.bfloat16)
        return carry

    early = rows // 8
    lax.fori_loop(0, early, project_other, 0)

    for d in range(1, group):
        near_copy(d, (lo + group - d) % group).wait_recv()

    valid = mask_ref[...] > 0
    for s in range(chans):
        keep = valid[:, s * span : (s + 1) * span].reshape(1, 1, span)
        for h in range(HEADS):
            part = blocks[:, s, h].astype(jnp.float32)
            bias[h, :, :, s * span : (s + 1) * span] = jnp.where(keep, part, NEVER)

    lane = lax.broadcasted_iota(jnp.int32, (span, width), 1) // head_dim

    def out_copy(i):
        return pltpu.make_async_copy(result.at[i], out_ref.at[i], out_sem.at[i])

    def attend(i, carry):
        query = queries[i]
        key = keys[i].reshape(total, width)
        value = values[i].reshape(total, 2 * width)
        top = jnp.zeros((span, width), jnp.float32)
        norm = jnp.zeros((span, width), jnp.float32)
        for h in range(HEADS):
            mine = jnp.where(lane == h, query, jnp.zeros_like(query))
            scores = lax.dot_general(mine, key, NT, preferred_element_type=jnp.float32)
            scores = scores + bias[h].reshape(span, total)
            peak = jnp.max(scores, axis=-1, keepdims=True)
            weights = jnp.exp2(scores - peak).astype(jnp.bfloat16)
            both = jnp.dot(weights, value, preferred_element_type=jnp.float32)
            top = jnp.where(lane == h, both[:, :width], top)
            norm = jnp.where(lane == h, both[:, width:], norm)
        high, low = halves(gates[i] * (top / norm))
        result[i] = jnp.dot(
            jnp.concatenate([high, low, high], axis=1),
            w_out[...],
            preferred_element_type=jnp.float32,
        )
        out_copy(i).start()
        return carry

    def attend_ahead(i, carry):
        project_other(i + early, carry)
        return attend(i, carry)

    lax.fori_loop(0, rows - early, attend_ahead, 0)
    lax.fori_loop(rows - early, rows, attend, 0)

    for g in range(chans):

        @pl.when(jnp.logical_or(hi != c, hi != g))
        def _():
            far_copy(g, c).wait_send()

    for d in range(1, group):
        near_copy(d, lo).wait_send()

    def finish(i, carry):
        for d in range(1, chans):
            x_copy(i, d, c).wait_send()
        out_copy(i).wait()
        return carry

    lax.fori_loop(0, rows, finish, 0)


def body(
    chans,
    pair_rep,
    residue_mask,
    norm_gain,
    norm_shift,
    proj_weight,
    gate_shift,
    bias_weight,
    out_weight,
):
    rows, span, width = pair_rep.shape
    group = span // rows
    total = chans * span
    vmem = pl.BlockSpec(memory_space=pltpu.VMEM)
    half = jnp.bfloat16
    full = jnp.float32
    return pl.pallas_call(
        functools.partial(kernel, chans, group),
        out_shape=jax.ShapeDtypeStruct((rows, span, width), full),
        in_specs=[vmem] * 8,
        out_specs=pl.BlockSpec(memory_space=pl.ANY),
        scratch_shapes=[
            pltpu.VMEM((rows, chans, span, width), half),
            pltpu.VMEM((group, chans, HEADS, rows, span), half),
            pltpu.VMEM((HEADS, rows, span), full),
            pltpu.VMEM((HEADS, rows, span), half),
            pltpu.VMEM((HEADS, group, rows, total), full),
            pltpu.VMEM((3 * width, 4 * width), half),
            pltpu.VMEM((2 * width, 2 * width), half),
            pltpu.VMEM((3 * width, width), half),
            pltpu.VMEM((rows, span, width), half),
            pltpu.VMEM((rows, span, width), half),
            pltpu.VMEM((rows, span, width), full),
            pltpu.VMEM((rows, chans, span, width), half),
            pltpu.VMEM((rows, chans, span, 2 * width), half),
            pltpu.VMEM((rows, span, width), full),
            pltpu.SemaphoreType.DMA((chans - 1, rows)),
            pltpu.SemaphoreType.DMA((chans - 1, rows)),
            pltpu.SemaphoreType.DMA((chans,)),
            pltpu.SemaphoreType.DMA((chans,)),
            pltpu.SemaphoreType.DMA((group - 1,)),
            pltpu.SemaphoreType.DMA((group - 1,)),
            pltpu.SemaphoreType.DMA((rows,)),
        ],
        compiler_params=pltpu.CompilerParams(
            collective_id=0, has_side_effects=True, vmem_limit_bytes=56 * 1024 * 1024
        ),
    )(
        pair_rep,
        residue_mask.reshape(1, total),
        norm_gain.reshape(1, width),
        norm_shift.reshape(1, width),
        proj_weight,
        gate_shift.reshape(1, width),
        bias_weight.T,
        out_weight,
    )


def solution(mesh):
    return jax.shard_map(
        functools.partial(body, mesh.shape["chan"]),
        mesh=mesh,
        in_specs=(P("row", "chan", None), P(), P(), P(), P(), P(), P(), P()),
        out_specs=P("row", "chan", None),
        check_vma=False,
    )
```
